32 devices in a mesh: depth: 4 (over z), rows: 8 (over y, x, core).
Axes of the slice: x: 2, y: 2, z: 4, core: 2. Of those that a mesh axis runs over, the one named last changes fastest.
Arguments:
- target: float32 [4, 2, 4096, 4096], P('depth', None, 'rows'), may hold values from -6 to 6
- depth_index: int32 [4], P('depth'), may hold values from 0 to 255
- band_mask: int32 [4, 2, 4096], P('depth'), may hold values from 0 to 1, as said below
Outputs:
- hologram: float32 [2, 4096, 4096], P(None, ('depth', 'rows'))
The draws below stay inside these ranges and needn't reach their ends.
Inputs may be any that keep to these rules, and one draw needn't show every extreme that they name: `band_mask`: for each plane and each of the two dimensions, the ones are exactly the frequency indices k with min(k, 4096 - k) below a cutoff between 512 and 2048.
All inputs are finite; a program needn't handle non-finite values.
Results may differ from the reference program's by a relative error of at most 0.0009.
Values sent between devices are 32-bit elements; how exact they have to be, the bound alone decides.
A program may use at most 128 MiB of HBM per device.

```python
import math
import jax
import jax.numpy as jnp
from jax import lax

N = 4096
PLANES = 4
DEPTHS = 256


def draw_band_mask(key, part):
    cutoff = jax.random.randint(key, (PLANES, 2, 1), N // 8, N // 2 + 1)
    indices = jnp.arange(N, dtype=jnp.int32)
    folded = jnp.minimum(indices, N - indices)
    return (folded[None, None, :] < cutoff).astype(jnp.int32)


def place_ends(values, key, low, top_value):
    spot = [jax.random.randint(jax.random.fold_in(key, axis), (), 0, length) for axis, length in enumerate(values.shape)]
    main_axis = values.shape.index(max(values.shape))
    neighbour = spot[:main_axis] + [(spot[main_axis] + 1) % values.shape[main_axis]] + spot[main_axis + 1:]
    return values.at[tuple(spot)].set(low).at[tuple(neighbour)].set(top_value)


def levels(stream_key, dims, cuts, low, top_value):
    loudness = 1.0
    for axis_at, parts in cuts:
        steps = jax.random.uniform(jax.random.fold_in(jax.random.fold_in(stream_key, 6), axis_at), (parts,), jnp.float32, low / len(cuts), top_value / len(cuts))
        loudness = loudness * jnp.repeat(jnp.exp(steps), dims[axis_at] // parts).reshape((-1,) + (1,) * (len(dims) - 1 - axis_at))
    return loudness


def normal_values(key, dims, width, reach, split=(), kind=jnp.bfloat16):
    result = jax.random.normal(key, dims, jnp.float32) * width
    if len(split) > 0:
        result = levels(key, dims, split, -0.22, 0.18) * result
    return jnp.clip(result, min=-reach, max=reach).astype(kind)


def setup_inputs(seed: int = 0) -> dict:
    key_of = jax.random.split(jax.random.key(seed), 4)
    return {
        "target": normal_values(key_of[0], (PLANES, 2, N, N), 1.0, 6.0, ((0, 4), (2, 8)), jnp.float32),
        "depth_index": place_ends(jax.random.randint(key_of[1], (PLANES,), 0, DEPTHS), jax.random.fold_in(key_of[1], 1), 0, DEPTHS - 1).astype(jnp.int32),
        "band_mask": draw_band_mask(jax.random.fold_in(key_of[3], 71), 0),
    }


def reference(target, depth_index, band_mask):
    planes_all = target.shape[0]
    indices = jnp.arange(N, dtype=jnp.int32)
    signed = jnp.where(indices < N // 2, indices, indices - N)
    frequency = signed.astype(jnp.float32) / N
    radical = jnp.sqrt(4.0 - frequency[:, None] ** 2 - frequency[None, :] ** 2)

    def add_plane(running_sum, inputs):
        plane_data, level_index, mask_pair = inputs
        wavefront = lax.complex(plane_data[0], plane_data[1])
        spectrum = jnp.fft.fft2(wavefront, norm='ortho')
        distance = 100.0 + 2.0 * level_index.astype(jnp.float32)
        phases = 2.0 * math.pi * distance * (radical - 2.0)
        weights = mask_pair[0].astype(jnp.float32)[:, None] * mask_pair[1].astype(jnp.float32)[None, :]
        rotated = spectrum * lax.complex(jnp.cos(phases) * weights, jnp.sin(phases) * weights)
        return (running_sum + rotated, None)
    zeros_real = jnp.zeros((N, N), dtype=jnp.float32)
    initial = lax.complex(zeros_real, zeros_real)
    summed, _ = lax.scan(add_plane, initial, (target, depth_index, band_mask))
    field_out = jnp.fft.ifft2(summed, norm='ortho') / jnp.sqrt(jnp.float32(planes_all))
    return jnp.stack([jnp.real(field_out), jnp.imag(field_out)]).astype(jnp.float32)
```

```python
import functools
import math

import jax
import jax.numpy as jnp
import numpy as np
from jax import lax
from jax.experimental import pallas as pl
from jax.experimental.pallas import tpu as pltpu
from jax.sharding import PartitionSpec as P

LOW = 32
HIGH = 128
N = LOW * HIGH
VMEM_LIMIT = 56 * 1024 * 1024


def scaled(value, factor_real, factor_imaginary):
    real, imaginary = value
    if abs(factor_imaginary) < 1e-12:
        if factor_real > 0:
            return (real, imaginary)
        return (-real, -imaginary)
    if abs(factor_real) < 1e-12:
        if factor_imaginary > 0:
            return (-imaginary, real)
        return (imaginary, -real)
    a, b = np.float32(factor_real), np.float32(factor_imaginary)
    return (real * a - imaginary * b, real * b + imaginary * a)


def root(numerator, length, direction):
    angle = direction * 2.0 * math.pi * (numerator % length) / length
    return math.cos(angle), math.sin(angle)


def add(left, right):
    return (left[0] + right[0], left[1] + right[1])


def subtract(left, right):
    return (left[0] - right[0], left[1] - right[1])


def butterfly(values, direction):
    count = len(values)
    if count == 1:
        return values
    even = butterfly(values[0::2], direction)
    odd = butterfly(values[1::2], direction)
    odd = [scaled(v, *root(k, count, direction)) for k, v in enumerate(odd)]
    return [add(e, o) for e, o in zip(even, odd)] + [subtract(e, o) for e, o in zip(even, odd)]


def dense_table(direction):
    index = np.arange(HIGH)
    angles = direction * 2.0 * np.pi / HIGH * (index[:, None] * index[None, :] % HIGH)
    cosine, sine = np.cos(angles), np.sin(angles)
    return np.block([[cosine, -sine], [sine, cosine]])


def halves(table):
    high = table.astype(np.float32).astype(jnp.bfloat16)
    low = (table - high.astype(np.float64)).astype(np.float32).astype(jnp.bfloat16)
    return jnp.asarray(high), jnp.asarray(low)


def twiddles(direction, scaling):
    product = np.arange(LOW)[:, None] * np.arange(HIGH)[None, :] % N
    angles = direction * 2.0 * np.pi / N * product
    return (
        jnp.asarray((np.cos(angles) * scaling).astype(np.float32)),
        jnp.asarray((np.sin(angles) * scaling).astype(np.float32)),
    )


def split(value):
    high = value.astype(jnp.bfloat16)
    return high, (value - high.astype(jnp.float32)).astype(jnp.bfloat16)


def dot(left, right):
    return jnp.dot(left, right, preferred_element_type=jnp.float32)


def width_kernel(chunk, chunks, owners, x_ref, tr_ref, ti_ref, th_ref, tl_ref, o_ref, hi_ref, lo_ref):
    tile = x_ref.shape[1]

    def body(step, carry):
        rows = pl.ds(pl.multiple_of(step * 16, 16), 16)
        values = []
        for first in range(owners):
            total = None
            for second in range(chunks):
                at = (first + owners * second) * HIGH
                value = (x_ref[0, rows, at:at + HIGH], x_ref[1, rows, at:at + HIGH])
                value = scaled(value, *root(chunk * second, chunks, -1.0))
                total = value if total is None else add(total, value)
            values.append(scaled(total, *root(chunk * first, LOW, -1.0)))
        for owner, (real, imaginary) in enumerate(butterfly(values, -1.0)):
            k = chunks * owner + chunk
            turn_real, turn_imaginary = tr_ref[k:k + 1, :], ti_ref[k:k + 1, :]
            high, low = split(real * turn_real - imaginary * turn_imaginary)
            hi_ref[owner, rows, :HIGH] = high
            lo_ref[owner, rows, :HIGH] = low
            high, low = split(real * turn_imaginary + imaginary * turn_real)
            hi_ref[owner, rows, HIGH:] = high
            lo_ref[owner, rows, HIGH:] = low
        return carry

    lax.fori_loop(0, tile // 16, body, 0)
    for owner in range(owners):
        high = hi_ref[owner]
        out = dot(high, th_ref[...]) + dot(lo_ref[owner], th_ref[...]) + dot(high, tl_ref[...])
        o_ref[owner, 0] = out[:, :HIGH]
        o_ref[owner, 1] = out[:, HIGH:]


def along_width(field, chunk, chunks, owners, tables):
    _, height, _ = field.shape
    tile = min(128, height)
    whole = lambda a: pl.BlockSpec(a.shape, lambda i: (0,) * a.ndim)
    return pl.pallas_call(
        functools.partial(width_kernel, chunk, chunks, owners),
        grid=(height // tile,),
        in_specs=[pl.BlockSpec((2, tile, N), lambda i: (0, i, 0))] + [whole(a) for a in tables],
        out_specs=pl.BlockSpec((owners, 2, tile, HIGH), lambda i: (0, 0, i, 0)),
        out_shape=jax.ShapeDtypeStruct((owners, 2, height, HIGH), jnp.float32),
        scratch_shapes=[pltpu.VMEM((owners, tile, 2 * HIGH), jnp.bfloat16)] * 2,
        compiler_params=pltpu.CompilerParams(vmem_limit_bytes=VMEM_LIMIT),
        cost_estimate=pl.CostEstimate(flops=6 * height * HIGH * HIGH * 4 * owners * 2, bytes_accessed=field.size * 4 + field.size * 4 // chunks, transcendentals=0),
        name=f"width_{chunk}",
    )(field, *tables)


def series(values, points):
    nodes = np.cos(np.pi * (np.arange(400) + 0.5) / 400) * 0.125 + 0.125
    basis = np.polynomial.chebyshev.Chebyshev.fit(nodes, values(np.sqrt(nodes)), points, domain=[0.0, 0.25])
    return [np.float32(c) for c in basis.convert(kind=np.polynomial.Polynomial).coef]


COSINE = series(lambda r: np.cos(2.0 * np.pi * r), 8)
SINE = series(lambda r: np.sin(2.0 * np.pi * r) / r, 8)


def horner(coefficients, at):
    total = coefficients[-1]
    for c in coefficients[-2::-1]:
        total = total * at + c
    return total


def signed(natural):
    return jnp.where(natural < N // 2, natural, natural - N).astype(jnp.float32)


def column_kernel(scalars_ref, x_ref, tr_ref, ti_ref, fh_ref, fl_ref, ih_ref, il_ref, o_ref, work_ref):
    owners, _, pieces, _, _ = x_ref.shape
    distance = scalars_ref[0].astype(jnp.float32) * 2.0 + 100.0
    limit_height = scalars_ref[1].astype(jnp.float32)
    limit_width = scalars_ref[2].astype(jnp.float32)
    column = scalars_ref[3]

    def forward(step, carry):
        rows = pl.ds(pl.multiple_of(step * 8, 8), 8)
        low_rows = pl.ds(pl.multiple_of(step * 8 + HIGH, 8), 8)
        values = [(x_ref[s, 0, p, rows, :], x_ref[s, 1, p, rows, :]) for s in range(owners) for p in range(pieces)]
        for k, (real, imaginary) in enumerate(butterfly(values, -1.0)):
            work_ref[k, rows, :] = real
            work_ref[k, low_rows, :] = imaginary
        return carry

    lax.fori_loop(0, HIGH // 8, forward, 0)

    across = signed(lax.broadcasted_iota(jnp.int32, (1, HIGH), 1) * LOW + column)
    inside_width = jnp.abs(across) < limit_width
    across_square = (across * (1.0 / N)) ** 2

    def turned(k, sign):
        real, imaginary = work_ref[k, :HIGH, :], work_ref[k, HIGH:, :]
        turn_real, turn_imaginary = tr_ref[k], ti_ref[k]
        return jnp.concatenate(
            [real * turn_real - imaginary * turn_imaginary, real * turn_imaginary + imaginary * turn_real], axis=0
        )

    def propagate(k, real, imaginary):
        down = signed(lax.broadcasted_iota(jnp.int32, (HIGH, HIGH), 0) * LOW + k)
        square = (down * (1.0 / N)) ** 2 + across_square
        turns = -distance * (square / (jnp.sqrt(4.0 - square) + 2.0))
        rest = turns - jnp.floor(turns + 0.5)
        at = rest * rest
        keep = jnp.logical_and(jnp.abs(down) < limit_height, inside_width)
        cosine = jnp.where(keep, horner(COSINE, at), 0.0)
        sine = jnp.where(keep, horner(SINE, at) * rest, 0.0)
        return jnp.concatenate([real * cosine - imaginary * sine, real * sine + imaginary * cosine], axis=0)

    def middle(step, carry):
        pair = [2 * step, 2 * step + 1]
        high, low = split(jnp.concatenate([turned(k, 1.0) for k in pair], axis=1))
        spectrum = dot(fh_ref[...], high) + dot(fh_ref[...], low) + dot(fl_ref[...], high)
        moved = [
            propagate(k, spectrum[:HIGH, i * HIGH:(i + 1) * HIGH], spectrum[HIGH:, i * HIGH:(i + 1) * HIGH])
            for i, k in enumerate(pair)
        ]
        high, low = split(jnp.concatenate(moved, axis=1))
        back = dot(ih_ref[...], high) + dot(ih_ref[...], low) + dot(il_ref[...], high)
        for i, k in enumerate(pair):
            real, imaginary = back[:HIGH, i * HIGH:(i + 1) * HIGH], back[HIGH:, i * HIGH:(i + 1) * HIGH]
            turn_real, turn_imaginary = tr_ref[k], ti_ref[k]
            work_ref[k, :HIGH, :] = real * turn_real + imaginary * turn_imaginary
            work_ref[k, HIGH:, :] = imaginary * turn_real - real * turn_imaginary
        return carry

    lax.fori_loop(0, LOW // 2, middle, 0)

    def inverse(step, carry):
        rows = pl.ds(pl.multiple_of(step * 8, 8), 8)
        low_rows = pl.ds(pl.multiple_of(step * 8 + HIGH, 8), 8)
        values = [(work_ref[k, rows, :], work_ref[k, low_rows, :]) for k in range(LOW)]
        for j, (real, imaginary) in enumerate(butterfly(values, 1.0)):
            o_ref[j, 0, rows, :] = real
            o_ref[j, 1, rows, :] = imaginary
        return carry

    lax.fori_loop(0, HIGH // 8, inverse, 0)


def columns_step(received, scalars, tables, chunk):
    owners, _, height, _ = received.shape
    received = received.reshape(owners, 2, height // HIGH, HIGH, HIGH)
    vmem = pl.BlockSpec(memory_space=pltpu.VMEM)
    return pl.pallas_call(
        column_kernel,
        in_specs=[pl.BlockSpec(memory_space=pltpu.SMEM)] + [vmem] * (1 + len(tables)),
        out_specs=vmem,
        out_shape=jax.ShapeDtypeStruct((LOW, 2, HIGH, HIGH), jnp.float32),
        scratch_shapes=[pltpu.VMEM((LOW, 2 * HIGH, HIGH), jnp.float32)],
        compiler_params=pltpu.CompilerParams(vmem_limit_bytes=VMEM_LIMIT),
        cost_estimate=pl.CostEstimate(flops=12 * LOW * HIGH * 256 * 256 * 2, bytes_accessed=16 * 1024 * 1024, transcendentals=0),
        name=f"column_{chunk}",
    )(scalars, received, *tables)


def output_kernel(chunks, *refs):
    inputs = refs[:chunks]
    tr_ref, ti_ref, th_ref, tl_ref, o_ref, work_ref = refs[chunks:]
    owners, _, height, _ = inputs[0].shape
    for owner in range(owners):
        for chunk in range(chunks):
            k = chunks * owner + chunk
            value = jnp.concatenate([inputs[chunk][owner, 0], inputs[chunk][owner, 1]], axis=1)
            high, low = split(value)
            out = dot(high, th_ref[...]) + dot(low, th_ref[...]) + dot(high, tl_ref[...])
            real, imaginary = out[:, :HIGH], out[:, HIGH:]
            turn_real, turn_imaginary = tr_ref[k:k + 1, :], ti_ref[k:k + 1, :]
            work_ref[k, 0] = real * turn_real - imaginary * turn_imaginary
            work_ref[k, 1] = real * turn_imaginary + imaginary * turn_real

    def body(step, carry):
        rows = pl.ds(pl.multiple_of(step * 8, 8), 8)
        values = [(work_ref[k, 0, rows, :], work_ref[k, 1, rows, :]) for k in range(LOW)]
        for j, (real, imaginary) in enumerate(butterfly(values, 1.0)):
            o_ref[0, rows, j * HIGH:(j + 1) * HIGH] = real
            o_ref[1, rows, j * HIGH:(j + 1) * HIGH] = imaginary
        return carry

    lax.fori_loop(0, height // 8, body, 0)


def inverse_width(parts, tables):
    height = parts[0].shape[2]
    vmem = pl.BlockSpec(memory_space=pltpu.VMEM)
    return pl.pallas_call(
        functools.partial(output_kernel, len(parts)),
        in_specs=[vmem] * (len(parts) + len(tables)),
        out_specs=vmem,
        out_shape=jax.ShapeDtypeStruct((2, height, N), jnp.float32),
        scratch_shapes=[pltpu.VMEM((LOW, 2, height, HIGH), jnp.float32)],
        compiler_params=pltpu.CompilerParams(vmem_limit_bytes=VMEM_LIMIT),
        cost_estimate=pl.CostEstimate(flops=6 * LOW * height * 256 * 256, bytes_accessed=8 * height * N * 2, transcendentals=0),
        name="output",
    )(*parts, *tables)


def local(target, depth_index, band_mask):
    owners, depths = lax.axis_size("rows"), lax.axis_size("depth")
    chunks = LOW // owners
    field = target.reshape(target.shape[1:])
    scale = 1.0 / math.sqrt(N)
    forward, backward = dense_table(-1.0), dense_table(1.0)
    forward_left, backward_left = halves(forward), halves(backward)
    forward_right, backward_right = halves(forward.T), halves(backward.T)
    turn = twiddles(-1.0, scale)
    turn_back = twiddles(1.0, scale / math.sqrt(depths))
    spread = tuple(jnp.broadcast_to(t[:, :, None], (LOW, HIGH, HIGH)) for t in turn)
    limits = (jnp.sum(band_mask[0], axis=-1) + 1) // 2
    me = lax.axis_index("rows")
    rows = N // (owners * depths)

    pieces = []
    for chunk in range(chunks):
        sent = along_width(field, chunk, chunks, owners, turn + forward_right)
        received = lax.all_to_all(sent, "rows", split_axis=0, concat_axis=0, tiled=True)
        scalars = jnp.stack([depth_index[0], limits[0], limits[1], me * chunks + chunk]).astype(jnp.int32)
        part = columns_step(received, scalars, spread + forward_left + backward_left, chunk)
        pieces.append(lax.psum_scatter(part, "depth", scatter_dimension=0, tiled=True))
    results = []
    for share in pieces:
        share = share.reshape(share.shape[0], 2, HIGH // rows, rows, HIGH)
        share = jnp.transpose(share, (0, 2, 1, 3, 4)).reshape(owners, 2, rows, HIGH)
        results.append(lax.all_to_all(share, "rows", split_axis=0, concat_axis=0, tiled=True))
    return inverse_width(results, turn_back + backward_right)


def solution(mesh):
    in_specs = (P("depth", None, "rows", None), P("depth"), P("depth", None, None))
    out_specs = P(None, ("depth", "rows"), None)
    return jax.shard_map(local, mesh=mesh, in_specs=in_specs, out_specs=out_specs, check_vma=False)
```

```python
import functools
import math

import jax
import jax.numpy as jnp
import numpy as np
from jax import lax
from jax.experimental import pallas as pl
from jax.experimental.pallas import tpu as pltpu
from jax.sharding import PartitionSpec as P


LOW = 32
HIGH = 128
N = LOW * HIGH
VMEM_LIMIT = 56 * 1024 * 1024


def scaled(value, factor_real, factor_imaginary):
    real, imaginary = value
    if abs(factor_imaginary) < 1e-12:
        if factor_real > 0:
            return (real, imaginary)
        return (-real, -imaginary)
    if abs(factor_real) < 1e-12:
        if factor_imaginary > 0:
            return (-imaginary, real)
        return (imaginary, -real)
    a, b = np.float32(factor_real), np.float32(factor_imaginary)
    return (real * a - imaginary * b, real * b + imaginary * a)


def root(numerator, length, direction):
    angle = direction * 2.0 * math.pi * (numerator % length) / length
    return math.cos(angle), math.sin(angle)


def add(left, right):
    return (left[0] + right[0], left[1] + right[1])


def subtract(left, right):
    return (left[0] - right[0], left[1] - right[1])


def butterfly(values, direction):
    count = len(values)
    if count == 1:
        return values
    even = butterfly(values[0::2], direction)
    odd = butterfly(values[1::2], direction)
    odd = [scaled(v, *root(k, count, direction)) for k, v in enumerate(odd)]
    return [add(e, o) for e, o in zip(even, odd)] + [subtract(e, o) for e, o in zip(even, odd)]


def dense_table(direction):
    index = np.arange(HIGH)
    angles = direction * 2.0 * np.pi / HIGH * (index[:, None] * index[None, :] % HIGH)
    cosine, sine = np.cos(angles), np.sin(angles)
    return np.block([[cosine, -sine], [sine, cosine]])


def halves(table):
    high = table.astype(np.float32).astype(jnp.bfloat16)
    low = (table - high.astype(np.float64)).astype(np.float32).astype(jnp.bfloat16)
    return jnp.asarray(high), jnp.asarray(low)


def twiddles(direction, scaling):
    product = np.arange(LOW)[:, None] * np.arange(HIGH)[None, :] % N
    angles = direction * 2.0 * np.pi / N * product
    return (
        jnp.asarray((np.cos(angles) * scaling).astype(np.float32)),
        jnp.asarray((np.sin(angles) * scaling).astype(np.float32)),
    )


def split(value):
    high = value.astype(jnp.bfloat16)
    return high, (value - high.astype(jnp.float32)).astype(jnp.bfloat16)


def tripled(value):
    high, low = split(value)
    return jnp.concatenate([high, low, high], axis=0)


def dot(left, right):
    return jnp.dot(left, right, preferred_element_type=jnp.float32)


def width_kernel(chunk, chunks, owners, x_ref, tr_ref, ti_ref, th_ref, tl_ref, o_ref, hi_ref, lo_ref):
    tile = x_ref.shape[1]

    def body(step, carry):
        rows = pl.ds(pl.multiple_of(step * 16, 16), 16)
        values = []
        for first in range(owners):
            total = None
            for second in range(chunks):
                at = (first + owners * second) * HIGH
                value = (x_ref[0, rows, at:at + HIGH], x_ref[1, rows, at:at + HIGH])
                value = scaled(value, *root(chunk * second, chunks, -1.0))
                total = value if total is None else add(total, value)
            values.append(scaled(total, *root(chunk * first, LOW, -1.0)))
        for owner, (real, imaginary) in enumerate(butterfly(values, -1.0)):
            k = chunks * owner + chunk
            turn_real, turn_imaginary = tr_ref[k:k + 1, :], ti_ref[k:k + 1, :]
            high, low = split(real * turn_real - imaginary * turn_imaginary)
            hi_ref[owner, rows, :HIGH] = high
            lo_ref[owner, rows, :HIGH] = low
            high, low = split(real * turn_imaginary + imaginary * turn_real)
            hi_ref[owner, rows, HIGH:] = high
            lo_ref[owner, rows, HIGH:] = low
        return carry

    lax.fori_loop(0, tile // 16, body, 0)
    for owner in range(owners):
        high = hi_ref[owner]
        out = dot(high, th_ref[...]) + dot(lo_ref[owner], th_ref[...]) + dot(high, tl_ref[...])
        o_ref[owner, 0] = out[:, :HIGH]
        o_ref[owner, 1] = out[:, HIGH:]


def along_width(field, chunk, chunks, owners, tables):
    _, height, _ = field.shape
    tile = min(128, height)
    whole = lambda a: pl.BlockSpec(a.shape, lambda i: (0,) * a.ndim)
    return pl.pallas_call(
        functools.partial(width_kernel, chunk, chunks, owners),
        grid=(height // tile,),
        in_specs=[pl.BlockSpec((2, tile, N), lambda i: (0, i, 0))] + [whole(a) for a in tables],
        out_specs=pl.BlockSpec((owners, 2, tile, HIGH), lambda i: (0, 0, i, 0)),
        out_shape=jax.ShapeDtypeStruct((owners, 2, height, HIGH), jnp.float32),
        scratch_shapes=[pltpu.VMEM((owners, tile, 2 * HIGH), jnp.bfloat16)] * 2,
        compiler_params=pltpu.CompilerParams(vmem_limit_bytes=VMEM_LIMIT),
        cost_estimate=pl.CostEstimate(flops=6 * height * HIGH * HIGH * 4 * owners * 2, bytes_accessed=field.size * 4 + field.size * 4 // chunks, transcendentals=0),
    )(field, *tables)


def series(values, points):
    nodes = np.cos(np.pi * (np.arange(400) + 0.5) / 400) * 0.125 + 0.125
    basis = np.polynomial.chebyshev.Chebyshev.fit(nodes, values(np.sqrt(nodes)), points, domain=[0.0, 0.25])
    return [np.float32(c) for c in basis.convert(kind=np.polynomial.Polynomial).coef]


COSINE = series(lambda r: np.cos(2.0 * np.pi * r), 6)
SINE = series(lambda r: np.sin(2.0 * np.pi * r) / r, 6)


def horner(coefficients, at):
    total = coefficients[-1]
    for c in coefficients[-2::-1]:
        total = total * at + c
    return total


def signed(natural):
    return jnp.where(natural < N // 2, natural, natural - N).astype(jnp.float32)


def column_kernel(scalars_ref, x_ref, tr_ref, ti_ref, f_ref, i_ref, o_ref, work_ref):
    owners, _, pieces, _, _ = x_ref.shape
    distance = scalars_ref[0].astype(jnp.float32) * 2.0 + 100.0
    limit_height = scalars_ref[1].astype(jnp.float32)
    limit_width = scalars_ref[2].astype(jnp.float32)
    column = scalars_ref[3]

    def forward(step, carry):
        rows = pl.ds(pl.multiple_of(step * 8, 8), 8)
        low_rows = pl.ds(pl.multiple_of(step * 8 + HIGH, 8), 8)
        values = [(x_ref[s, 0, p, rows, :], x_ref[s, 1, p, rows, :]) for s in range(owners) for p in range(pieces)]
        for k, (real, imaginary) in enumerate(butterfly(values, -1.0)):
            work_ref[k, rows, :] = real
            work_ref[k, low_rows, :] = imaginary
        return carry

    lax.fori_loop(0, HIGH // 8, forward, 0)

    across = signed(lax.broadcasted_iota(jnp.int32, (1, HIGH), 1) * LOW + column)
    inside_width = jnp.abs(across) < limit_width
    across_square = (across * (1.0 / N)) ** 2

    def turned(k):
        real, imaginary = work_ref[k, :HIGH, :], work_ref[k, HIGH:, :]
        turn_real, turn_imaginary = tr_ref[k], ti_ref[k]
        return jnp.concatenate(
            [real * turn_real - imaginary * turn_imaginary, real * turn_imaginary + imaginary * turn_real], axis=0
        )

    def propagate(k, real, imaginary):
        down = signed(lax.broadcasted_iota(jnp.int32, (HIGH, HIGH), 0) * LOW + k)
        square = (down * (1.0 / N)) ** 2 + across_square
        rest_square = 4.0 - square
        drop = 2.0 - rest_square * lax.rsqrt(rest_square)
        turns = -distance * (0.25 * (square + drop * drop))
        rest = turns - jnp.floor(turns + 0.5)
        at = rest * rest
        keep = jnp.logical_and(jnp.abs(down) < limit_height, inside_width)
        cosine = jnp.where(keep, horner(COSINE, at), 0.0)
        sine = jnp.where(keep, horner(SINE, at) * rest, 0.0)
        return jnp.concatenate([real * cosine - imaginary * sine, real * sine + imaginary * cosine], axis=0)

    def middle(step, carry):
        pair = [2 * step, 2 * step + 1]
        spectrum = dot(f_ref[...], tripled(jnp.concatenate([turned(k) for k in pair], axis=1)))
        moved = [
            propagate(k, spectrum[:HIGH, i * HIGH:(i + 1) * HIGH], spectrum[HIGH:, i * HIGH:(i + 1) * HIGH])
            for i, k in enumerate(pair)
        ]
        back = dot(i_ref[...], tripled(jnp.concatenate(moved, axis=1)))
        for i, k in enumerate(pair):
            real, imaginary = back[:HIGH, i * HIGH:(i + 1) * HIGH], back[HIGH:, i * HIGH:(i + 1) * HIGH]
            turn_real, turn_imaginary = tr_ref[k], ti_ref[k]
            work_ref[k, :HIGH, :] = real * turn_real + imaginary * turn_imaginary
            work_ref[k, HIGH:, :] = imaginary * turn_real - real * turn_imaginary
        return carry

    lax.fori_loop(0, LOW // 2, middle, 0)

    def inverse(step, carry):
        rows = pl.ds(pl.multiple_of(step * 8, 8), 8)
        low_rows = pl.ds(pl.multiple_of(step * 8 + HIGH, 8), 8)
        values = [(work_ref[k, rows, :], work_ref[k, low_rows, :]) for k in range(LOW)]
        for j, (real, imaginary) in enumerate(butterfly(values, 1.0)):
            o_ref[j, 0, rows, :] = real
            o_ref[j, 1, rows, :] = imaginary
        return carry

    lax.fori_loop(0, HIGH // 8, inverse, 0)


def columns_step(received, scalars, tables):
    owners, _, height, _ = received.shape
    received = received.reshape(owners, 2, height // HIGH, HIGH, HIGH)
    vmem = pl.BlockSpec(memory_space=pltpu.VMEM)
    return pl.pallas_call(
        column_kernel,
        in_specs=[pl.BlockSpec(memory_space=pltpu.SMEM)] + [vmem] * (1 + len(tables)),
        out_specs=vmem,
        out_shape=jax.ShapeDtypeStruct((LOW, 2, HIGH, HIGH), jnp.float32),
        scratch_shapes=[pltpu.VMEM((LOW, 2 * HIGH, HIGH), jnp.float32)],
        compiler_params=pltpu.CompilerParams(vmem_limit_bytes=VMEM_LIMIT),
        cost_estimate=pl.CostEstimate(flops=12 * LOW * HIGH * 256 * 256 * 2, bytes_accessed=16 * 1024 * 1024, transcendentals=0),
    )(scalars, received, *tables)


def output_kernel(chunks, *refs):
    inputs = refs[:chunks]
    tr_ref, ti_ref, th_ref, tl_ref, o_ref, work_ref = refs[chunks:]
    owners, _, height, _ = inputs[0].shape
    for owner in range(owners):
        for chunk in range(chunks):
            k = chunks * owner + chunk
            value = jnp.concatenate([inputs[chunk][owner, 0], inputs[chunk][owner, 1]], axis=1)
            high, low = split(value)
            out = dot(high, th_ref[...]) + dot(low, th_ref[...]) + dot(high, tl_ref[...])
            real, imaginary = out[:, :HIGH], out[:, HIGH:]
            turn_real, turn_imaginary = tr_ref[k:k + 1, :], ti_ref[k:k + 1, :]
            work_ref[k, 0] = real * turn_real - imaginary * turn_imaginary
            work_ref[k, 1] = real * turn_imaginary + imaginary * turn_real

    def body(step, carry):
        rows = pl.ds(pl.multiple_of(step * 8, 8), 8)
        values = [(work_ref[k, 0, rows, :], work_ref[k, 1, rows, :]) for k in range(LOW)]
        for j, (real, imaginary) in enumerate(butterfly(values, 1.0)):
            o_ref[0, rows, j * HIGH:(j + 1) * HIGH] = real
            o_ref[1, rows, j * HIGH:(j + 1) * HIGH] = imaginary
        return carry

    lax.fori_loop(0, height // 8, body, 0)


def inverse_width(parts, tables):
    height = parts[0].shape[2]
    vmem = pl.BlockSpec(memory_space=pltpu.VMEM)
    return pl.pallas_call(
        functools.partial(output_kernel, len(parts)),
        in_specs=[vmem] * (len(parts) + len(tables)),
        out_specs=vmem,
        out_shape=jax.ShapeDtypeStruct((2, height, N), jnp.float32),
        scratch_shapes=[pltpu.VMEM((LOW, 2, height, HIGH), jnp.float32)],
        compiler_params=pltpu.CompilerParams(vmem_limit_bytes=VMEM_LIMIT),
        cost_estimate=pl.CostEstimate(flops=6 * LOW * height * 256 * 256, bytes_accessed=8 * height * N * 2, transcendentals=0),
        name="output",
    )(*parts, *tables)


def local(target, depth_index, band_mask):
    owners, depths = lax.axis_size("rows"), lax.axis_size("depth")
    chunks = LOW // owners
    field = target.reshape(target.shape[1:])
    scale = 1.0 / math.sqrt(N)
    forward, backward = dense_table(-1.0), dense_table(1.0)
    left = tuple(jnp.concatenate([h, h, l], axis=1) for h, l in (halves(forward), halves(backward)))
    forward_right, backward_right = halves(forward.T), halves(backward.T)
    turn = twiddles(-1.0, scale)
    turn_back = twiddles(1.0, scale / math.sqrt(depths))
    spread = tuple(jnp.broadcast_to(t[:, :, None], (LOW, HIGH, HIGH)) for t in turn)
    limits = (jnp.sum(band_mask[0], axis=-1) + 1) // 2
    me = lax.axis_index("rows")
    rows = N // (owners * depths)

    pieces = []
    for chunk in range(chunks):
        sent = along_width(field, chunk, chunks, owners, turn + forward_right)
        received = lax.all_to_all(sent, "rows", split_axis=0, concat_axis=0, tiled=True)
        scalars = jnp.stack([depth_index[0], limits[0], limits[1], me * chunks + chunk]).astype(jnp.int32)
        part = columns_step(received, scalars, spread + left)
        pieces.append(lax.psum_scatter(part, "depth", scatter_dimension=0, tiled=True))
    results = []
    for share in pieces:
        share = share.reshape(share.shape[0], 2, HIGH // rows, rows, HIGH)
        share = jnp.transpose(share, (0, 2, 1, 3, 4)).reshape(owners, 2, rows, HIGH)
        results.append(lax.all_to_all(share, "rows", split_axis=0, concat_axis=0, tiled=True))
    return inverse_width(results, turn_back + backward_right)


def solution(mesh):
    in_specs = (P("depth", None, "rows", None), P("depth"), P("depth", None, None))
    out_specs = P(None, ("depth", "rows"), None)
    return jax.shard_map(local, mesh=mesh, in_specs=in_specs, out_specs=out_specs, check_vma=False)
```
